32 devices in a mesh: hot: 4 (over z), cold: 8 (over y, x, core).
Axes of the slice: x: 2, y: 2, z: 4, core: 2. Of those that a mesh axis runs over, the one named last changes fastest.
Arguments:
- tokens: bfloat16 [128, 8192], P('cold', 'hot'), may hold values from -6 to 6
- hot_gate: bfloat16 [8192, 1024], P('hot', 'cold'), may hold values from -0.0625 to 0.0625
- hot_up: bfloat16 [8192, 1024], P('hot', 'cold'), may hold values from -0.0625 to 0.0625
- hot_down: bfloat16 [1024, 8192], P('cold', 'hot'), may hold values from -0.125 to 0.125
- cold_gate: bfloat16 [8192, 6144], P('hot', 'cold'), may hold values from -0.0625 to 0.0625
- cold_up: bfloat16 [8192, 6144], P('hot', 'cold'), may hold values from -0.0625 to 0.0625
- cold_down: bfloat16 [6144, 8192], P('cold', 'hot'), may hold values from -0.125 to 0.125
- hot_ids: int32 [8], replicated, may hold values from 0 to 55, as said below
- cold_ids: int32 [48], replicated, may hold values from 0 to 55, as said below
- block_mask: int32 [128, 56], replicated, may hold values from 0 to 1, as said below
Outputs:
- mixed: bfloat16 [128, 8192], P('cold', 'hot')
The draws below stay inside these ranges and needn't reach their ends.
Inputs may be any that keep to these rules, and one draw needn't show every extreme that they name: hot_ids and cold_ids together name every block number from 0 to 55 once. `cold_ids`: cold slot s lies with index s // 6 of cold. `block_mask`: among the 16 tokens of one index of cold, at most 8 have a 1 in a cold slot of one given index of cold; in every draw some index of cold gets exactly 8 such tokens from every index of cold.
All inputs are finite; a program needn't handle non-finite values.
Results may differ from the reference program's by a relative error of at most 0.0049.
Values may be sent and summed in bfloat16 or wider, within the bound.
A program may use at most 64 MiB of HBM per device.

```python
import jax
import jax.numpy as jnp
from jax import lax

D = 8192
BLOCK = 128
COLD_DEV = 6
TOK_DEV = 16
CAP = 8
TOKENS = 128
HB = 8
CB = 48
NB = 56
FF = 7168
N_COLD = 8


def rank_tokens(rank_key):
    return jax.random.permutation(rank_key, TOK_DEV).astype(jnp.int32)


def routing_tables(key):
    folded = jax.random.fold_in(key, 41)
    subkeys = jax.random.split(folded, 11)
    middle = (jax.random.permutation(subkeys[0], NB - 2) + 1).astype(jnp.int32)
    hot_list = jnp.concatenate([middle[:HB - 1], jnp.zeros((1,), jnp.int32)])
    cold_list = jnp.concatenate([middle[HB - 1:], jnp.full((1,), NB - 1, jnp.int32)])
    hot_ids = jnp.take(hot_list, jax.random.permutation(subkeys[9], HB).astype(jnp.int32))
    cold_ids = jnp.take(cold_list, jax.random.permutation(subkeys[10], CB).astype(jnp.int32))
    group_total = CB // COLD_DEV
    sources = TOKENS // TOK_DEV
    group_level = jax.random.randint(subkeys[1], (group_total,), 1, 5)
    busy_group = jax.random.randint(subkeys[2], (), 0, group_total)
    ceiling = group_level * CAP // 4
    hit_count = jax.random.randint(subkeys[3], (sources, group_total), 0, ceiling[None, :] + 1)
    hit_count = jnp.where(jnp.arange(group_total)[None, :] == busy_group, CAP, hit_count)
    rank_keys = jax.random.split(subkeys[4], sources * group_total)
    token_ranks = jax.vmap(rank_tokens)(rank_keys).reshape(sources, group_total, TOK_DEV)
    group_hit = token_ranks < hit_count[:, :, None]
    first_block = jax.random.randint(subkeys[5], (sources, group_total, TOK_DEV), 0, COLD_DEV)
    extra_blocks = jax.random.randint(subkeys[6], (sources, group_total, TOK_DEV, COLD_DEV), 0, 4) == 0
    chosen_blocks = (first_block[..., None] == jnp.arange(COLD_DEV)) | extra_blocks
    chosen_blocks = chosen_blocks & group_hit[..., None]
    cold_mask = jnp.transpose(chosen_blocks, (0, 2, 1, 3)).reshape(TOKENS, CB).astype(jnp.int32)
    hot_rate = jax.random.randint(subkeys[7], (HB,), 5, 10)
    hot_mask = (jax.random.randint(subkeys[8], (TOKENS, HB), 0, 10) < hot_rate[None, :]).astype(jnp.int32)
    block_mask = jnp.zeros((TOKENS, NB), jnp.int32)
    block_mask = block_mask.at[:, hot_ids].set(hot_mask)
    block_mask = block_mask.at[:, cold_ids].set(cold_mask)
    return (hot_ids, cold_ids, block_mask)


def draw_hot_ids(key, part):
    return routing_tables(key)[0]


def draw_cold_ids(key, part):
    return routing_tables(key)[1]


def draw_block_mask(key, part):
    return routing_tables(key)[2]


def steps_of(stream_key, dims, shards, low, high):
    gain, own = 1.0, jax.random.fold_in(stream_key, 6)
    for axis_at, parts in shards:
        heights = jnp.exp(jax.random.uniform(jax.random.fold_in(own, axis_at), (parts,), jnp.float32, low / len(shards), high / len(shards)))
        gain = gain * jnp.repeat(heights, dims[axis_at] // parts).reshape([-1 if axis == axis_at else 1 for axis in range(len(dims))])
    return gain


def scatter_about(own_key, shape, spread, bound, pieces=(), kind=jnp.bfloat16):
    result = spread * jax.random.normal(own_key, shape, jnp.float32)
    if pieces:
        result = result * steps_of(own_key, shape, pieces, -0.22, 0.18)
    return jnp.clip(result, -bound, bound).astype(kind)


def setup_inputs(seed: int = 0) -> dict:
    arg_keys = jax.random.split(jax.random.key(seed), 11)
    tokens = scatter_about(arg_keys[0], (TOKENS, D), 1.0, 6.0, ((0, 8), (1, 4)))
    hot_gate = scatter_about(arg_keys[1], (D, HB * BLOCK), D ** -0.5, 0.0625, ((0, 4), (1, 8)))
    hot_up = scatter_about(arg_keys[2], (D, HB * BLOCK), D ** -0.5, 0.0625, ((0, 4), (1, 8)))
    hot_down = scatter_about(arg_keys[3], (HB * BLOCK, D), (FF // 4) ** -0.5, 0.125, ((0, 8), (1, 4)))
    cold_gate = scatter_about(arg_keys[4], (D, CB * BLOCK), D ** -0.5, 0.0625, ((0, 4), (1, 8)))
    cold_up = scatter_about(arg_keys[5], (D, CB * BLOCK), D ** -0.5, 0.0625, ((0, 4), (1, 8)))
    cold_down = scatter_about(arg_keys[6], (CB * BLOCK, D), (FF // 4) ** -0.5, 0.125, ((0, 8), (1, 4)))
    hot_ids = draw_hot_ids(jax.random.fold_in(arg_keys[10], 71), 0)
    cold_ids = draw_cold_ids(jax.random.fold_in(arg_keys[10], 71), 0)
    block_mask = draw_block_mask(jax.random.fold_in(arg_keys[10], 71), 0)
    return dict(tokens=tokens, hot_gate=hot_gate, hot_up=hot_up, hot_down=hot_down, cold_gate=cold_gate, cold_up=cold_up, cold_down=cold_down, hot_ids=hot_ids, cold_ids=cold_ids, block_mask=block_mask)


def ranged_product(matrix_rows, weight):
    return jnp.dot(matrix_rows, weight, preferred_element_type=jnp.float32)


def reference(tokens, hot_gate, hot_up, hot_down, cold_gate, cold_up, cold_down, hot_ids, cold_ids, block_mask):
    hot_bits = jnp.take(block_mask, hot_ids, axis=1)
    cold_bits = jnp.take(block_mask, cold_ids, axis=1)
    hot_gates = ranged_product(tokens, hot_gate)
    hot_ups = ranged_product(tokens, hot_up)
    hot_scale = jnp.repeat(hot_bits.astype(jnp.float32), BLOCK, axis=1)
    hot_hidden = (jax.nn.silu(hot_gates) * hot_ups * hot_scale).astype(jnp.bfloat16)
    hot_out = jnp.dot(hot_hidden, hot_down, preferred_element_type=jnp.float32)
    padded_tokens = jnp.concatenate([tokens, jnp.zeros((1, D), tokens.dtype)], axis=0)
    span = COLD_DEV * BLOCK

    def add_group(running, group_index):
        group_bits = lax.dynamic_slice_in_dim(cold_bits, (group_index * COLD_DEV).astype(jnp.int32), COLD_DEV, 1)
        group_hit = jnp.max(group_bits, axis=1) > 0
        picked = jnp.nonzero(group_hit, size=N_COLD * CAP, fill_value=TOKENS)[0].astype(jnp.int32)
        padded_bits = jnp.concatenate([group_bits, jnp.zeros((1, COLD_DEV), group_bits.dtype)], axis=0)
        picked_rows = jnp.take(padded_tokens, picked, axis=0)
        picked_bits = jnp.take(padded_bits, picked, axis=0)
        first_col = (group_index * span).astype(jnp.int32)
        gate_part = lax.dynamic_slice_in_dim(cold_gate, first_col, span, 1)
        up_part = lax.dynamic_slice_in_dim(cold_up, first_col, span, 1)
        down_part = lax.dynamic_slice_in_dim(cold_down, first_col, span, 0)
        gate_sum = ranged_product(picked_rows, gate_part)
        up_sum = ranged_product(picked_rows, up_part)
        scale = jnp.repeat(picked_bits.astype(jnp.float32), BLOCK, axis=1)
        hidden = (jax.nn.silu(gate_sum) * up_sum * scale).astype(jnp.bfloat16)
        group_out = jnp.dot(hidden, down_part, preferred_element_type=jnp.float32)
        return running.at[picked].add(group_out), None

    initial = jnp.zeros((TOKENS + 1, D), jnp.float32)
    cold_out = lax.scan(add_group, initial, jnp.arange(N_COLD, dtype=jnp.int32))[0]
    return (hot_out + cold_out[:TOKENS]).astype(jnp.bfloat16)
```

```python
import functools

import jax
import jax.numpy as jnp
from jax import lax
from jax.experimental import pallas as pl
from jax.experimental.pallas import tpu as pltpu
from jax.sharding import PartitionSpec as P

BLOCK = 128
CHUNK = 256
OUT_CHUNK = 512
MESH = pl.DeviceIdType.MESH
NT = (((1,), (1,)), ((), ()))
SUM_TYPE = jnp.float32
OUT_TYPE = jnp.bfloat16


def dot(a, b):
    return jnp.dot(a, b, preferred_element_type=jnp.float32)


def dot_nt(a, b):
    return lax.dot_general(a, b, NT, preferred_element_type=jnp.float32)


def zero_one(condition):
    return jnp.where(condition, 1.0, 0.0).astype(jnp.bfloat16)


def hidden_of(sums, bits, first_slot):
    width = sums.shape[1] // 2
    gate, up = sums[:, :width], sums[:, width:]
    value = gate / (1.0 + jnp.exp(-gate)) * up
    pieces = [
        value[:, j * BLOCK:(j + 1) * BLOCK] * bits[:, first_slot + j:first_slot + j + 1]
        for j in range(width // BLOCK)
    ]
    return jnp.concatenate(pieces, axis=1).astype(jnp.bfloat16)


def kernel(
    n_hot, n_cold,
    tok_in, hg_in, hu_in, hd_in, cg_in, cu_in, cd_in, hid_in, cid_in, mask_in,
    out_ref,
    tok_all, w_hot, w_cold, w_down, hot_ids, cold_ids, mask,
    picked, bits_hot, bits_cold, spread,
    part_hot, part_cold, send_hot, send_cold, got_hot, got_cold,
    own_hot, own_cold, full, outs, pair_in, mine, ready, final_in,
    load_sem, tok_sem, tok_send, tok_recv, fwd_send, fwd_recv,
    rs_send, rs_recv, hg_send, hg_recv, pr_send, pr_recv, fin_send, fin_recv,
):
    me_hot, me_cold = lax.axis_index("hot"), lax.axis_index("cold")
    pairs = n_cold // 2
    my_pair, my_side = me_cold // 2, me_cold % 2
    other = my_pair * 2 + (1 - my_side)
    rows = tok_in.shape[0]
    tokens = tok_all.shape[0]
    hot_width = hg_in.shape[1]
    hot_slots = hot_width // BLOCK
    cold_width = cg_in.shape[1]
    cold_slots = cold_width // BLOCK
    chunks = cold_width // CHUNK
    slot_count = rows // 2
    picks = n_cold * slot_count
    hot_rows, cold_rows = tokens // n_hot, picks // n_hot
    cols = tok_in.shape[1]
    out_chunks = cols // OUT_CHUNK

    own_slot = tok_all.at[pl.ds(pl.multiple_of(me_cold * rows, rows), rows)]
    tok_load = pltpu.make_async_copy(tok_in, own_slot, tok_sem)
    tok_load.start()
    loads = []

    def load(src, dst):
        copy = pltpu.make_async_copy(src, dst, load_sem.at[len(loads)])
        copy.start()
        loads.append(copy)

    load(hid_in, hot_ids)
    load(cid_in, cold_ids)
    load(mask_in, mask)
    load(hg_in, w_hot.at[:, pl.ds(0, hot_width)])
    load(hu_in, w_hot.at[:, pl.ds(hot_width, hot_width)])
    for k in range(chunks):
        load(cg_in.at[:, pl.ds(k * CHUNK, CHUNK)], w_cold.at[k, :, pl.ds(0, CHUNK)])
        load(cu_in.at[:, pl.ds(k * CHUNK, CHUNK)], w_cold.at[k, :, pl.ds(CHUNK, CHUNK)])
    load(hd_in, w_down.at[pl.ds(0, hot_width)])
    load(cd_in, w_down.at[pl.ds(hot_width, cold_width)])

    barrier = pltpu.get_barrier_semaphore()
    hot_peers = [lax.rem(me_hot + k, n_hot) for k in range(1, n_hot)]
    pair_peers = [lax.rem(my_pair + k, pairs) for k in range(1, pairs)]
    for peer in hot_peers:
        pl.semaphore_signal(barrier, inc=1, device_id={"hot": peer}, device_id_type=MESH)
    for peer in pair_peers:
        pl.semaphore_signal(
            barrier, inc=1, device_id={"cold": peer * 2 + my_side}, device_id_type=MESH
        )
    pl.semaphore_signal(barrier, inc=1, device_id={"cold": other}, device_id_type=MESH)
    pl.semaphore_wait(barrier, n_hot - 1 + pairs - 1 + 1)

    sent = []

    def send(src, dst, s_sem, r_sem, device):
        copy = pltpu.make_async_remote_copy(
            src_ref=src, dst_ref=dst, send_sem=s_sem, recv_sem=r_sem,
            device_id=device, device_id_type=MESH,
        )
        copy.start()
        sent.append(copy)

    def arrive(dst, s_sem, r_sem, device):
        pltpu.make_async_remote_copy(
            src_ref=dst, dst_ref=dst, send_sem=s_sem, recv_sem=r_sem,
            device_id=device, device_id_type=MESH,
        ).wait_recv()

    tok_load.wait()
    for k, peer in enumerate(pair_peers):
        send(own_slot, own_slot, tok_send.at[k], tok_recv.at[my_pair],
             {"cold": peer * 2 + my_side})
    send(own_slot, own_slot, fwd_send.at[0], fwd_recv.at[my_pair], {"cold": other})

    for copy in loads[:3]:
        copy.wait()
    slots_pad = bits_hot.shape[1]
    blocks = mask.shape[1]
    slot_at = lax.broadcasted_iota(jnp.int32, (slots_pad, blocks), 0)
    id_at = jnp.full((slots_pad, blocks), -1, jnp.int32)
    for j in range(hot_slots):
        id_at = jnp.where(slot_at == j, hot_ids[me_cold * hot_slots + j], id_at)
    for j in range(cold_slots):
        id_at = jnp.where(slot_at == hot_slots + j, cold_ids[me_cold * cold_slots + j], id_at)
    chosen = zero_one(lax.broadcasted_iota(jnp.int32, (slots_pad, blocks), 1) == id_at)
    mask_value = mask[...].astype(jnp.float32).astype(jnp.bfloat16)
    bits_t = dot_nt(chosen, mask_value)
    slot_row = lax.broadcasted_iota(jnp.int32, (slots_pad, tokens), 0)
    is_cold = (slot_row >= hot_slots) & (slot_row < hot_slots + cold_slots)
    hit = jnp.max(jnp.where(is_cold, bits_t, 0.0), axis=0, keepdims=True)

    def group_of(shape, dim):
        at = lax.broadcasted_iota(jnp.int32, shape, dim)
        total = jnp.zeros(shape, jnp.int32)
        for g in range(1, n_cold):
            total = total + jnp.where(at >= g * rows, 1, 0)
        return total

    group_row, group_col = group_of((1, tokens), 1), group_of((tokens, 1), 0)
    before = lax.broadcasted_iota(jnp.int32, (tokens, tokens), 0) < lax.broadcasted_iota(
        jnp.int32, (tokens, tokens), 1
    )
    before = zero_one(before & (group_row == group_col))
    rank = dot(jnp.broadcast_to(hit, (8, tokens)).astype(jnp.bfloat16), before)[0:1]
    target = jnp.where(hit > 0.5, group_row * slot_count + rank.astype(jnp.int32), -1)
    pick = zero_one(lax.broadcasted_iota(jnp.int32, (picks, tokens), 0) == target)
    eye = zero_one(
        lax.broadcasted_iota(jnp.int32, (tokens, tokens), 0)
        == lax.broadcasted_iota(jnp.int32, (tokens, tokens), 1)
    )
    spread[...] = dot_nt(eye, pick).astype(jnp.bfloat16)
    bits_cold[...] = dot_nt(pick, bits_t.astype(jnp.bfloat16))
    bits_hot[...] = dot_nt(mask_value, chosen)

    def slot_of(device):
        return tok_all.at[pl.ds(pl.multiple_of(device * rows, rows), rows)]

    for k in range(1, pairs):
        source = lax.rem(my_pair + pairs - k, pairs)
        slot = slot_of(source * 2 + my_side)
        arrive(slot, tok_send.at[k - 1], tok_recv.at[source], {"cold": source * 2 + my_side})
        send(slot, slot, fwd_send.at[k], fwd_recv.at[source], {"cold": other})
    for k in range(pairs):
        source = lax.rem(my_pair + pairs - k, pairs)
        arrive(slot_of(source * 2 + (1 - my_side)), fwd_send.at[k], fwd_recv.at[source],
               {"cold": other})

    def part(index, value, kept, outgoing, incoming, count):
        kept[...] = value
        if outgoing is not kept:
            outgoing[...] = value.astype(outgoing.dtype)
        for k, peer in enumerate(hot_peers):
            send(
                outgoing.at[pl.ds(pl.multiple_of(peer * count, count), count)],
                incoming.at[me_hot],
                rs_send.at[index, k], rs_recv.at[index, me_hot], {"hot": peer},
            )

    loads[3].wait()
    loads[4].wait()
    picked[...] = dot(pick, tok_all[...]).astype(jnp.bfloat16)
    for k in range(chunks):
        loads[5 + 2 * k].wait()
        loads[6 + 2 * k].wait()
        part(k, dot(picked[...], w_cold[k]), part_cold.at[k], send_cold.at[k],
             got_cold.at[k], cold_rows)
    part(chunks, dot(tok_all[...], w_hot[...]), part_hot, send_hot, got_hot, hot_rows)

    def finish(index, kept, incoming, count, bits, first_slot, held):
        own = pl.ds(pl.multiple_of(me_hot * count, count), count)
        total = kept[own]
        for k in range(1, n_hot):
            source = lax.rem(me_hot + n_hot - k, n_hot)
            arrive(incoming.at[source], rs_send.at[index, k - 1], rs_recv.at[index, source],
                   {"hot": source})
            total = total + incoming[source].astype(jnp.float32)
        held[own] = hidden_of(total, bits[own], first_slot)
        for k, peer in enumerate(hot_peers):
            send(held.at[own], held.at[own], hg_send.at[index, k], hg_recv.at[index, me_hot],
                 {"hot": peer})

    for k in range(chunks):
        finish(k, part_cold.at[k], got_cold.at[k], cold_rows, bits_cold,
               hot_slots + k * (CHUNK // BLOCK), own_cold.at[k])
    finish(chunks, part_hot, got_hot, hot_rows, bits_hot, 0, own_hot)

    def gathered(index, count, held):
        for k in range(1, n_hot):
            source = lax.rem(me_hot + n_hot - k, n_hot)
            arrive(held.at[pl.ds(pl.multiple_of(source * count, count), count)],
                   hg_send.at[index, k - 1], hg_recv.at[index, source], {"hot": source})

    for k in range(chunks):
        gathered(k, cold_rows, own_cold.at[k])
        full[:, hot_width + k * CHUNK:hot_width + (k + 1) * CHUNK] = dot(
            spread[...], own_cold[k]
        ).astype(jnp.bfloat16)
    gathered(chunks, hot_rows, own_hot)
    full[:, :hot_width] = own_hot[...]

    for copy in loads[5 + 2 * chunks:]:
        copy.wait()
    for c in range(out_chunks):
        at = pl.ds(c * OUT_CHUNK, OUT_CHUNK)
        value = dot(full[...], w_down[:, c * OUT_CHUNK:(c + 1) * OUT_CHUNK])
        outs[:, :, :, at] = value.reshape(pairs, 2, rows, OUT_CHUNK)
        send(outs.at[:, 1 - my_side, :, at], pair_in.at[:, :, at],
             pr_send.at[c], pr_recv.at[c], {"cold": other})
    for c in range(out_chunks):
        at = pl.ds(c * OUT_CHUNK, OUT_CHUNK)
        arrive(pair_in.at[:, :, at], pr_send.at[c], pr_recv.at[c], {"cold": other})
        value = outs[:, my_side, :, at] + pair_in[:, :, at]
        mine[:, :, at] = value
        ready[:, :, at] = value.astype(ready.dtype)
        for k, peer in enumerate(pair_peers):
            send(ready.at[peer, :, at], final_in.at[my_pair, :, at],
                 fin_send.at[c, k], fin_recv.at[c, my_pair], {"cold": peer * 2 + my_side})
    for c in range(out_chunks):
        at = pl.ds(c * OUT_CHUNK, OUT_CHUNK)
        total = mine[my_pair, :, at]
        for k in range(1, pairs):
            source = lax.rem(my_pair + pairs - k, pairs)
            arrive(final_in.at[source, :, at], fin_send.at[c, k - 1], fin_recv.at[c, source],
                   {"cold": source * 2 + my_side})
            total = total + final_in[source, :, at].astype(jnp.float32)
        out_ref[:, at] = total.astype(out_ref.dtype)
    for copy in sent:
        copy.wait_send()


def body(n_hot, n_cold, *args):
    (tokens, hot_gate, hot_up, hot_down, cold_gate, cold_up, cold_down,
     hot_ids, cold_ids, block_mask) = args
    rows, cols = tokens.shape
    total_rows = block_mask.shape[0]
    hot_width, cold_width = hot_gate.shape[1], cold_gate.shape[1]
    chunks = cold_width // CHUNK
    picks = n_cold * (rows // 2)
    pairs = n_cold // 2
    slots_pad = -(-((hot_width + cold_width) // BLOCK) // 8) * 8
    hot_rows, cold_rows = total_rows // n_hot, picks // n_hot
    out_chunks = cols // OUT_CHUNK
    bf16, f32, i32 = jnp.bfloat16, jnp.float32, jnp.int32
    vmem, dma = pltpu.VMEM, pltpu.SemaphoreType.DMA
    scratch = [
        vmem((total_rows, cols), bf16),
        vmem((cols, 2 * hot_width), bf16),
        vmem((chunks, cols, 2 * CHUNK), bf16),
        vmem((hot_width + cold_width, cols), bf16),
        pltpu.SMEM(hot_ids.shape, i32),
        pltpu.SMEM(cold_ids.shape, i32),
        vmem(block_mask.shape, i32),
        vmem((picks, cols), bf16),
        vmem((total_rows, slots_pad), f32),
        vmem((picks, slots_pad), f32),
        vmem((total_rows, picks), bf16),
        vmem((total_rows, 2 * hot_width), f32),
        vmem((chunks, picks, 2 * CHUNK), f32),
        vmem((total_rows, 2 * hot_width), SUM_TYPE),
        vmem((chunks, picks, 2 * CHUNK), SUM_TYPE),
        vmem((n_hot, hot_rows, 2 * hot_width), SUM_TYPE),
        vmem((chunks, n_hot, cold_rows, 2 * CHUNK), SUM_TYPE),
        vmem((total_rows, hot_width), bf16),
        vmem((chunks, picks, CHUNK), bf16),
        vmem((total_rows, hot_width + cold_width), bf16),
        vmem((pairs, 2, rows, cols), f32),
        vmem((pairs, rows, cols), f32),
        vmem((pairs, rows, cols), f32),
        vmem((pairs, rows, cols), OUT_TYPE),
        vmem((pairs, rows, cols), OUT_TYPE),
        dma((7 + 2 * chunks,)),
        dma,
        dma((pairs,)),
        dma((pairs,)),
        dma((pairs,)),
        dma((pairs,)),
        dma((chunks + 1, n_hot)),
        dma((chunks + 1, n_hot)),
        dma((chunks + 1, n_hot)),
        dma((chunks + 1, n_hot)),
        dma((out_chunks,)),
        dma((out_chunks,)),
        dma((out_chunks, pairs)),
        dma((out_chunks, pairs)),
    ]
    return pl.pallas_call(
        functools.partial(kernel, n_hot, n_cold),
        out_shape=jax.ShapeDtypeStruct((rows, cols), bf16),
        in_specs=[pl.BlockSpec(memory_space=pl.ANY)] * 10,
        out_specs=pl.BlockSpec(memory_space=pltpu.VMEM),
        scratch_shapes=scratch,
        compiler_params=pltpu.CompilerParams(
            collective_id=0, has_side_effects=True, vmem_limit_bytes=60 * 1024 * 1024
        ),
        name="decode_step",
    )(*args)


def solution(mesh):
    return jax.shard_map(
        functools.partial(body, mesh.shape["hot"], mesh.shape["cold"]),
        mesh=mesh,
        in_specs=(
            P("cold", "hot"),
            P("hot", "cold"),
            P("hot", "cold"),
            P("cold", "hot"),
            P("hot", "cold"),
            P("hot", "cold"),
            P("cold", "hot"),
            P(),
            P(),
            P(),
        ),
        out_specs=P("cold", "hot"),
        check_vma=False,
    )
```

```python
import functools

import jax
import jax.numpy as jnp
from jax import lax
from jax.experimental import pallas as pl
from jax.experimental.pallas import tpu as pltpu
from jax.sharding import PartitionSpec as P

BLOCK = 128
CHUNK = 256
OUT_CHUNK = 512
MESH = pl.DeviceIdType.MESH
NT = (((1,), (1,)), ((), ()))
SUM_TYPE = jnp.bfloat16
OUT_TYPE = jnp.bfloat16


def dot(a, b):
    return jnp.dot(a, b, preferred_element_type=jnp.float32)


def dot_nt(a, b):
    return lax.dot_general(a, b, NT, preferred_element_type=jnp.float32)


def zero_one(condition):
    return jnp.where(condition, 1.0, 0.0).astype(jnp.bfloat16)


def hidden_of(sums, bits, first_slot):
    width = sums.shape[1] // 2
    gate, up = sums[:, :width], sums[:, width:]
    value = gate / (1.0 + jnp.exp(-gate)) * up
    pieces = [
        value[:, j * BLOCK:(j + 1) * BLOCK] * bits[:, first_slot + j:first_slot + j + 1]
        for j in range(width // BLOCK)
    ]
    return jnp.concatenate(pieces, axis=1).astype(jnp.bfloat16)


def kernel(
    n_hot, n_cold,
    tok_in, hg_in, hu_in, hd_in, cg_in, cu_in, cd_in, hid_in, cid_in, mask_in,
    out_ref,
    tok_all, w_hot, w_cold, w_down, hot_ids, cold_ids, mask,
    picked, bits_hot, bits_cold, spread,
    part_hot, part_cold, send_hot, send_cold, got_hot, got_cold,
    own_hot, own_cold, full, outs, pair_in, mine, ready, final_in,
    load_sem, tok_sem, tok_send, tok_recv, fwd_send, fwd_recv,
    rs_send, rs_recv, hg_send, hg_recv, pr_send, pr_recv, fin_send, fin_recv,
):
    me_hot, me_cold = lax.axis_index("hot"), lax.axis_index("cold")
    pairs = n_cold // 2
    my_pair, my_side = me_cold // 2, me_cold % 2
    other = my_pair * 2 + (1 - my_side)
    rows = tok_in.shape[0]
    tokens = tok_all.shape[0]
    hot_width = hg_in.shape[1]
    hot_slots = hot_width // BLOCK
    cold_width = cg_in.shape[1]
    cold_slots = cold_width // BLOCK
    chunks = cold_width // CHUNK
    slot_count = rows // 2
    picks = n_cold * slot_count
    hot_rows, cold_rows = tokens // n_hot, picks // n_hot
    cols = tok_in.shape[1]
    out_chunks = cols // OUT_CHUNK

    own_slot = tok_all.at[pl.ds(pl.multiple_of(me_cold * rows, rows), rows)]
    tok_load = pltpu.make_async_copy(tok_in, own_slot, tok_sem)
    tok_load.start()
    loads = []

    def load(src, dst):
        copy = pltpu.make_async_copy(src, dst, load_sem.at[len(loads)])
        copy.start()
        loads.append(copy)

    load(hid_in, hot_ids)
    load(cid_in, cold_ids)
    load(mask_in, mask)
    load(hg_in, w_hot.at[:, pl.ds(0, hot_width)])
    load(hu_in, w_hot.at[:, pl.ds(hot_width, hot_width)])
    for k in range(chunks):
        load(cg_in.at[:, pl.ds(k * CHUNK, CHUNK)], w_cold.at[k, :, pl.ds(0, CHUNK)])
        load(cu_in.at[:, pl.ds(k * CHUNK, CHUNK)], w_cold.at[k, :, pl.ds(CHUNK, CHUNK)])
    load(hd_in, w_down.at[pl.ds(0, hot_width)])
    load(cd_in, w_down.at[pl.ds(hot_width, cold_width)])

    barrier = pltpu.get_barrier_semaphore()
    hot_peers = [lax.rem(me_hot + k, n_hot) for k in range(1, n_hot)]
    pair_peers = [lax.rem(my_pair + k, pairs) for k in range(1, pairs)]
    for peer in hot_peers:
        pl.semaphore_signal(barrier, inc=1, device_id={"hot": peer}, device_id_type=MESH)
    for peer in pair_peers:
        pl.semaphore_signal(
            barrier, inc=1, device_id={"cold": peer * 2 + my_side}, device_id_type=MESH
        )
    pl.semaphore_signal(barrier, inc=1, device_id={"cold": other}, device_id_type=MESH)
    pl.semaphore_wait(barrier, n_hot - 1 + pairs - 1 + 1)

    sent = []

    def send(src, dst, s_sem, r_sem, device):
        copy = pltpu.make_async_remote_copy(
            src_ref=src, dst_ref=dst, send_sem=s_sem, recv_sem=r_sem,
            device_id=device, device_id_type=MESH,
        )
        copy.start()
        sent.append(copy)

    def arrive(dst, s_sem, r_sem, device):
        pltpu.make_async_remote_copy(
            src_ref=dst, dst_ref=dst, send_sem=s_sem, recv_sem=r_sem,
            device_id=device, device_id_type=MESH,
        ).wait_recv()

    tok_load.wait()
    for k, peer in enumerate(pair_peers):
        send(own_slot, own_slot, tok_send.at[k], tok_recv.at[my_pair],
             {"cold": peer * 2 + my_side})
    send(own_slot, own_slot, fwd_send.at[0], fwd_recv.at[my_pair], {"cold": other})

    for copy in loads[:3]:
        copy.wait()
    slots_pad = bits_hot.shape[1]
    blocks = mask.shape[0]
    slot_at = lax.broadcasted_iota(jnp.int32, (slots_pad, blocks), 0)
    id_at = jnp.full((slots_pad, blocks), -1, jnp.int32)
    for j in range(hot_slots):
        id_at = jnp.where(slot_at == j, hot_ids[me_cold * hot_slots + j], id_at)
    for j in range(cold_slots):
        id_at = jnp.where(slot_at == hot_slots + j, cold_ids[me_cold * cold_slots + j], id_at)
    chosen = zero_one(lax.broadcasted_iota(jnp.int32, (slots_pad, blocks), 1) == id_at)
    mask_value = mask[...].astype(jnp.float32).astype(jnp.bfloat16)
    bits_t = dot(chosen, mask_value)
    slot_row = lax.broadcasted_iota(jnp.int32, (slots_pad, tokens), 0)
    is_cold = (slot_row >= hot_slots) & (slot_row < hot_slots + cold_slots)
    hit = jnp.max(jnp.where(is_cold, bits_t, 0.0), axis=0, keepdims=True)

    def group_of(shape, dim):
        at = lax.broadcasted_iota(jnp.int32, shape, dim)
        total = jnp.zeros(shape, jnp.int32)
        for g in range(1, n_cold):
            total = total + jnp.where(at >= g * rows, 1, 0)
        return total

    group_row, group_col = group_of((1, tokens), 1), group_of((tokens, 1), 0)
    before = lax.broadcasted_iota(jnp.int32, (tokens, tokens), 0) < lax.broadcasted_iota(
        jnp.int32, (tokens, tokens), 1
    )
    before = zero_one(before & (group_row == group_col))
    rank = dot(jnp.broadcast_to(hit, (8, tokens)).astype(jnp.bfloat16), before)[0:1]
    target = jnp.where(hit > 0.5, group_row * slot_count + rank.astype(jnp.int32), -1)
    pick = zero_one(lax.broadcasted_iota(jnp.int32, (picks, tokens), 0) == target)
    eye = zero_one(
        lax.broadcasted_iota(jnp.int32, (tokens, tokens), 0)
        == lax.broadcasted_iota(jnp.int32, (tokens, tokens), 1)
    )
    spread[...] = dot_nt(eye, pick).astype(jnp.bfloat16)
    bits_cold[...] = dot_nt(pick, bits_t.astype(jnp.bfloat16))
    bits_hot[...] = dot_nt(eye, bits_t.astype(jnp.bfloat16))

    def slot_of(device):
        return tok_all.at[pl.ds(pl.multiple_of(device * rows, rows), rows)]

    for k in range(1, pairs):
        source = lax.rem(my_pair + pairs - k, pairs)
        slot = slot_of(source * 2 + my_side)
        arrive(slot, tok_send.at[k - 1], tok_recv.at[source], {"cold": source * 2 + my_side})
        send(slot, slot, fwd_send.at[k], fwd_recv.at[source], {"cold": other})
    for k in range(pairs):
        source = lax.rem(my_pair + pairs - k, pairs)
        arrive(slot_of(source * 2 + (1 - my_side)), fwd_send.at[k], fwd_recv.at[source],
               {"cold": other})

    def part(index, value, kept, outgoing, incoming, count):
        kept[...] = value
        if outgoing is not kept:
            outgoing[...] = value.astype(outgoing.dtype)
        for k, peer in enumerate(hot_peers):
            send(
                outgoing.at[pl.ds(pl.multiple_of(peer * count, count), count)],
                incoming.at[me_hot],
                rs_send.at[index, k], rs_recv.at[index, me_hot], {"hot": peer},
            )

    loads[3].wait()
    loads[4].wait()
    picked[...] = dot(pick, tok_all[...]).astype(jnp.bfloat16)
    for k in range(chunks):
        loads[5 + 2 * k].wait()
        loads[6 + 2 * k].wait()
        part(k, dot(picked[...], w_cold[k]), part_cold.at[k], send_cold.at[k],
             got_cold.at[k], cold_rows)
    part(chunks, dot(tok_all[...], w_hot[...]), part_hot, send_hot, got_hot, hot_rows)

    def finish(index, kept, incoming, count, bits, first_slot, held):
        own = pl.ds(pl.multiple_of(me_hot * count, count), count)
        total = kept[own]
        for k in range(1, n_hot):
            source = lax.rem(me_hot + n_hot - k, n_hot)
            arrive(incoming.at[source], rs_send.at[index, k - 1], rs_recv.at[index, source],
                   {"hot": source})
            total = total + incoming[source].astype(jnp.float32)
        held[own] = hidden_of(total, bits[own], first_slot)
        for k, peer in enumerate(hot_peers):
            send(held.at[own], held.at[own], hg_send.at[index, k], hg_recv.at[index, me_hot],
                 {"hot": peer})

    for k in range(chunks):
        finish(k, part_cold.at[k], got_cold.at[k], cold_rows, bits_cold,
               hot_slots + k * (CHUNK // BLOCK), own_cold.at[k])
    finish(chunks, part_hot, got_hot, hot_rows, bits_hot, 0, own_hot)

    def gathered(index, count, held):
        for k in range(1, n_hot):
            source = lax.rem(me_hot + n_hot - k, n_hot)
            arrive(held.at[pl.ds(pl.multiple_of(source * count, count), count)],
                   hg_send.at[index, k - 1], hg_recv.at[index, source], {"hot": source})

    for k in range(chunks):
        gathered(k, cold_rows, own_cold.at[k])
        full[:, hot_width + k * CHUNK:hot_width + (k + 1) * CHUNK] = dot(
            spread[...], own_cold[k]
        ).astype(jnp.bfloat16)
    gathered(chunks, hot_rows, own_hot)
    full[:, :hot_width] = own_hot[...]

    for copy in loads[5 + 2 * chunks:]:
        copy.wait()
    for c in range(out_chunks):
        at = pl.ds(c * OUT_CHUNK, OUT_CHUNK)
        value = dot(full[...], w_down[:, c * OUT_CHUNK:(c + 1) * OUT_CHUNK])
        outs[:, :, :, at] = value.reshape(pairs, 2, rows, OUT_CHUNK)
        send(outs.at[:, 1 - my_side, :, at], pair_in.at[:, :, at],
             pr_send.at[c], pr_recv.at[c], {"cold": other})
    for c in range(out_chunks):
        at = pl.ds(c * OUT_CHUNK, OUT_CHUNK)
        arrive(pair_in.at[:, :, at], pr_send.at[c], pr_recv.at[c], {"cold": other})
        value = outs[:, my_side, :, at] + pair_in[:, :, at]
        mine[:, :, at] = value
        ready[:, :, at] = value.astype(ready.dtype)
        for k, peer in enumerate(pair_peers):
            send(ready.at[peer, :, at], final_in.at[my_pair, :, at],
                 fin_send.at[c, k], fin_recv.at[c, my_pair], {"cold": peer * 2 + my_side})
    for c in range(out_chunks):
        at = pl.ds(c * OUT_CHUNK, OUT_CHUNK)
        total = mine[my_pair, :, at]
        for k in range(1, pairs):
            source = lax.rem(my_pair + pairs - k, pairs)
            arrive(final_in.at[source, :, at], fin_send.at[c, k - 1], fin_recv.at[c, source],
                   {"cold": source * 2 + my_side})
            total = total + final_in[source, :, at].astype(jnp.float32)
        out_ref[:, at] = total.astype(out_ref.dtype)
    for copy in sent:
        copy.wait_send()


def body(n_hot, n_cold, *args):
    (tokens, hot_gate, hot_up, hot_down, cold_gate, cold_up, cold_down,
     hot_ids, cold_ids, block_mask) = args
    rows, cols = tokens.shape
    total_rows = block_mask.shape[0]
    hot_width, cold_width = hot_gate.shape[1], cold_gate.shape[1]
    chunks = cold_width // CHUNK
    picks = n_cold * (rows // 2)
    pairs = n_cold // 2
    slots_pad = -(-((hot_width + cold_width) // BLOCK) // 8) * 8
    hot_rows, cold_rows = total_rows // n_hot, picks // n_hot
    out_chunks = cols // OUT_CHUNK
    bf16, f32, i32 = jnp.bfloat16, jnp.float32, jnp.int32
    vmem, dma = pltpu.VMEM, pltpu.SemaphoreType.DMA
    scratch = [
        vmem((total_rows, cols), bf16),
        vmem((cols, 2 * hot_width), bf16),
        vmem((chunks, cols, 2 * CHUNK), bf16),
        vmem((hot_width + cold_width, cols), bf16),
        pltpu.SMEM(hot_ids.shape, i32),
        pltpu.SMEM(cold_ids.shape, i32),
        vmem(block_mask.shape[::-1], i32),
        vmem((picks, cols), bf16),
        vmem((total_rows, slots_pad), f32),
        vmem((picks, slots_pad), f32),
        vmem((total_rows, picks), bf16),
        vmem((total_rows, 2 * hot_width), f32),
        vmem((chunks, picks, 2 * CHUNK), f32),
        vmem((total_rows, 2 * hot_width), SUM_TYPE),
        vmem((chunks, picks, 2 * CHUNK), SUM_TYPE),
        vmem((n_hot, hot_rows, 2 * hot_width), SUM_TYPE),
        vmem((chunks, n_hot, cold_rows, 2 * CHUNK), SUM_TYPE),
        vmem((total_rows, hot_width), bf16),
        vmem((chunks, picks, CHUNK), bf16),
        vmem((total_rows, hot_width + cold_width), bf16),
        vmem((pairs, 2, rows, cols), f32),
        vmem((pairs, rows, cols), f32),
        vmem((pairs, rows, cols), f32),
        vmem((pairs, rows, cols), OUT_TYPE),
        vmem((pairs, rows, cols), OUT_TYPE),
        dma((7 + 2 * chunks,)),
        dma,
        dma((pairs,)),
        dma((pairs,)),
        dma((pairs,)),
        dma((pairs,)),
        dma((chunks + 1, n_hot)),
        dma((chunks + 1, n_hot)),
        dma((chunks + 1, n_hot)),
        dma((chunks + 1, n_hot)),
        dma((out_chunks,)),
        dma((out_chunks,)),
        dma((out_chunks, pairs)),
        dma((out_chunks, pairs)),
    ]
    return pl.pallas_call(
        functools.partial(kernel, n_hot, n_cold),
        out_shape=jax.ShapeDtypeStruct((rows, cols), bf16),
        in_specs=[pl.BlockSpec(memory_space=pl.ANY)] * 10,
        out_specs=pl.BlockSpec(memory_space=pltpu.VMEM),
        scratch_shapes=scratch,
        compiler_params=pltpu.CompilerParams(
            collective_id=0, has_side_effects=True, vmem_limit_bytes=60 * 1024 * 1024
        ),
        name="decode_step",
    )(*args[:-1], block_mask.T)


def solution(mesh):
    return jax.shard_map(
        functools.partial(body, mesh.shape["hot"], mesh.shape["cold"]),
        mesh=mesh,
        in_specs=(
            P("cold", "hot"),
            P("hot", "cold"),
            P("hot", "cold"),
            P("cold", "hot"),
            P("hot", "cold"),
            P("hot", "cold"),
            P("cold", "hot"),
            P(),
            P(),
            P(),
        ),
        out_specs=P("cold", "hot"),
        check_vma=False,
    )
```

```python
import functools

import jax
import jax.numpy as jnp
from jax import lax
from jax.experimental import pallas as pl
from jax.experimental.pallas import tpu as pltpu
from jax.sharding import PartitionSpec as P

BLOCK = 128
CHUNK = 384
OUT_CHUNK = 1024
MESH = pl.DeviceIdType.MESH
NT = (((1,), (1,)), ((), ()))
SUM_TYPE = jnp.bfloat16
OUT_TYPE = jnp.bfloat16


def dot(a, b):
    return jnp.dot(a, b, preferred_element_type=jnp.float32)


def dot_nt(a, b):
    return lax.dot_general(a, b, NT, preferred_element_type=jnp.float32)


def zero_one(condition):
    return jnp.where(condition, 1.0, 0.0).astype(jnp.bfloat16)


def hidden_of(sums, bits, first_slot):
    width = sums.shape[1] // 2
    gate, up = sums[:, :width], sums[:, width:]
    value = gate / (1.0 + jnp.exp(-gate)) * up
    pieces = [
        value[:, j * BLOCK:(j + 1) * BLOCK] * bits[:, first_slot + j:first_slot + j + 1]
        for j in range(width // BLOCK)
    ]
    return jnp.concatenate(pieces, axis=1).astype(jnp.bfloat16)


def kernel(
    n_hot, n_cold,
    tok_in, hg_in, hu_in, hd_in, cg_in, cu_in, cd_in, hid_in, cid_in, mask_in,
    out_ref,
    tok_all, w_hot, w_cold, w_down, hot_ids, cold_ids, mask,
    picks_of, picked, bits_hot, bits_cold, spread,
    part_hot, part_cold, send_hot, send_cold, got_hot, got_cold,
    own_hot, own_cold, full, outs, pair_in, mine, ready, final_in,
    load_sem, tok_sem, tok_send, tok_recv, fwd_send, fwd_recv,
    rs_send, rs_recv, hg_send, hg_recv, pr_send, pr_recv, fin_send, fin_recv,
):
    me_hot, me_cold = lax.axis_index("hot"), lax.axis_index("cold")
    pairs = n_cold // 2
    span = pairs // 2
    my_pair, my_side = me_cold // 2, me_cold % 2
    my_half, my_place = my_pair // span, my_pair % span
    halves = (my_half, 1 - my_half)
    other = my_pair * 2 + (1 - my_side)
    rows = tok_in.shape[0]
    stage_tokens = tok_all.shape[0] // 2
    hot_width = hg_in.shape[1]
    hot_slots = hot_width // BLOCK
    cold_width = cg_in.shape[1]
    cold_slots = cold_width // BLOCK
    chunks = cold_width // CHUNK
    slot_count = rows // 2
    stage_picks = (n_cold // 2) * slot_count
    hot_rows, cold_rows = stage_tokens // n_hot, stage_picks // n_hot
    cols = tok_in.shape[1]
    out_chunks = cols // OUT_CHUNK

    own_slot = tok_all.at[pl.ds(pl.multiple_of(me_cold * rows, rows), rows)]
    tok_load = pltpu.make_async_copy(tok_in, own_slot, tok_sem)
    tok_load.start()
    loads = []

    def load(src, dst):
        copy = pltpu.make_async_copy(src, dst, load_sem.at[len(loads)])
        copy.start()
        loads.append(copy)

    def load_cold(k):
        load(cg_in.at[:, pl.ds(k * CHUNK, CHUNK)], w_cold.at[k, :, pl.ds(0, CHUNK)])
        load(cu_in.at[:, pl.ds(k * CHUNK, CHUNK)], w_cold.at[k, :, pl.ds(CHUNK, CHUNK)])

    load(hid_in, hot_ids)
    load(cid_in, cold_ids)
    load(mask_in, mask)
    load_cold(0)

    barrier = pltpu.get_barrier_semaphore()
    hot_peers = [lax.rem(me_hot + k, n_hot) for k in range(1, n_hot)]
    near_places = [lax.rem(my_place + k, span) for k in range(1, span)]
    far_places = [lax.rem(my_place + k, span) for k in range(span)]
    places = (near_places, far_places)
    pair_peers = [my_half * span + at for at in near_places]
    pair_peers += [(1 - my_half) * span + at for at in far_places]
    sources = [my_half * span + lax.rem(my_place + span - k, span) for k in range(1, span)]
    sources += [(1 - my_half) * span + lax.rem(my_place + span - k, span) for k in range(span)]
    for peer in hot_peers:
        pl.semaphore_signal(barrier, inc=1, device_id={"hot": peer}, device_id_type=MESH)
    for peer in pair_peers:
        pl.semaphore_signal(
            barrier, inc=1, device_id={"cold": peer * 2 + my_side}, device_id_type=MESH
        )
    pl.semaphore_signal(barrier, inc=1, device_id={"cold": other}, device_id_type=MESH)
    pl.semaphore_wait(barrier, n_hot - 1 + pairs - 1 + 1)

    sent = []

    def send(src, dst, s_sem, r_sem, device):
        copy = pltpu.make_async_remote_copy(
            src_ref=src, dst_ref=dst, send_sem=s_sem, recv_sem=r_sem,
            device_id=device, device_id_type=MESH,
        )
        copy.start()
        sent.append(copy)

    def arrive(dst, s_sem, r_sem, device):
        pltpu.make_async_remote_copy(
            src_ref=dst, dst_ref=dst, send_sem=s_sem, recv_sem=r_sem,
            device_id=device, device_id_type=MESH,
        ).wait_recv()

    tok_load.wait()
    for k, peer in enumerate(pair_peers):
        send(own_slot, own_slot, tok_send.at[k], tok_recv.at[my_pair],
             {"cold": peer * 2 + my_side})
    send(own_slot, own_slot, fwd_send.at[0], fwd_recv.at[my_pair], {"cold": other})
    for k in range(1, chunks):
        load_cold(k)
    load(hg_in, w_hot.at[:, pl.ds(0, hot_width)])
    load(hu_in, w_hot.at[:, pl.ds(hot_width, hot_width)])
    load(hd_in, w_down.at[pl.ds(0, hot_width)])
    load(cd_in, w_down.at[pl.ds(hot_width, cold_width)])

    for copy in loads[:3]:
        copy.wait()
    slots_pad = bits_hot.shape[-1]
    blocks = mask.shape[0]
    slot_at = lax.broadcasted_iota(jnp.int32, (slots_pad, blocks), 0)
    id_at = jnp.full((slots_pad, blocks), -1, jnp.int32)
    for j in range(hot_slots):
        id_at = jnp.where(slot_at == j, hot_ids[me_cold * hot_slots + j], id_at)
    for j in range(cold_slots):
        id_at = jnp.where(slot_at == hot_slots + j, cold_ids[me_cold * cold_slots + j], id_at)
    chosen = zero_one(lax.broadcasted_iota(jnp.int32, (slots_pad, blocks), 1) == id_at)
    mask_value = mask[...].astype(jnp.float32).astype(jnp.bfloat16)
    all_bits = dot(chosen, mask_value)

    def group_of(shape, dim):
        at = lax.broadcasted_iota(jnp.int32, shape, dim)
        total = jnp.zeros(shape, jnp.int32)
        for g in range(1, n_cold // 2):
            total = total + jnp.where(at >= g * rows, 1, 0)
        return total

    square = (stage_tokens, stage_tokens)
    row_at = lax.broadcasted_iota(jnp.int32, square, 0)
    col_at = lax.broadcasted_iota(jnp.int32, square, 1)
    group_row, group_col = group_of((1, stage_tokens), 1), group_of((stage_tokens, 1), 0)
    before = zero_one((row_at < col_at) & (group_row == group_col))
    eye = zero_one(row_at == col_at)
    slot_row = lax.broadcasted_iota(jnp.int32, (slots_pad, stage_tokens), 0)
    is_cold = (slot_row >= hot_slots) & (slot_row < hot_slots + cold_slots)
    pick_at = lax.broadcasted_iota(jnp.int32, (stage_picks, stage_tokens), 0)
    for s in range(2):
        bits_t = jnp.where(
            halves[s] == 0, all_bits[:, :stage_tokens], all_bits[:, stage_tokens:]
        )
        hit = jnp.max(jnp.where(is_cold, bits_t, 0.0), axis=0, keepdims=True)
        rank = dot(jnp.broadcast_to(hit, (8, stage_tokens)).astype(jnp.bfloat16), before)[0:1]
        target = jnp.where(hit > 0.5, group_row * slot_count + rank.astype(jnp.int32), -1)
        pick = zero_one(pick_at == target)
        picks_of[s] = pick
        spread[s] = dot_nt(eye, pick).astype(jnp.bfloat16)
        narrow = bits_t.astype(jnp.bfloat16)
        bits_cold[s] = dot_nt(pick, narrow).reshape(n_hot, cold_rows, slots_pad)
        bits_hot[s] = dot_nt(eye, narrow).reshape(n_hot, hot_rows, slots_pad)

    def slot_of(device):
        return tok_all.at[pl.ds(pl.multiple_of(device * rows, rows), rows)]

    def forward(which):
        for k in which:
            source = sources[k]
            slot = slot_of(source * 2 + my_side)
            arrive(slot, tok_send.at[k], tok_recv.at[source], {"cold": source * 2 + my_side})
            send(slot, slot, fwd_send.at[k + 1], fwd_recv.at[source], {"cold": other})

    def forwarded(which):
        for k in which:
            source = my_pair if k < 0 else sources[k]
            arrive(slot_of(source * 2 + (1 - my_side)), fwd_send.at[k + 1], fwd_recv.at[source],
                   {"cold": other})

    def part(s, index, value, kept, outgoing, incoming):
        value = value.reshape(kept.shape)
        kept[...] = value
        outgoing[...] = value.astype(outgoing.dtype)
        for k, peer in enumerate(hot_peers):
            send(outgoing.at[peer], incoming.at[me_hot],
                 rs_send.at[s, index, k], rs_recv.at[s, index, me_hot], {"hot": peer})

    def parts(s):
        here = tok_all.at[pl.ds(pl.multiple_of(halves[s] * stage_tokens, stage_tokens), stage_tokens)]
        picked[s] = dot(picks_of[s], here[...]).astype(jnp.bfloat16)
        for k in range(chunks):
            if s == 0:
                loads[3 + 2 * k].wait()
                loads[4 + 2 * k].wait()
            part(s, k, dot(picked[s], w_cold[k]), part_cold.at[s, k], send_cold.at[s, k],
                 got_cold.at[s, k])
        if s == 0:
            forward(range(span - 1, pairs - 1))
            loads[3 + 2 * chunks].wait()
            loads[4 + 2 * chunks].wait()
        part(s, chunks, dot(here[...], w_hot[...]), part_hot.at[s], send_hot.at[s], got_hot.at[s])

    forward(range(span - 1))
    forwarded(range(-1, span - 1))
    parts(0)
    forwarded(range(span - 1, pairs - 1))
    parts(1)

    def finish(s, index, kept, incoming, bits, first_slot, held):
        total = kept[me_hot]
        for k in range(1, n_hot):
            source = lax.rem(me_hot + n_hot - k, n_hot)
            arrive(incoming.at[source], rs_send.at[s, index, k - 1],
                   rs_recv.at[s, index, source], {"hot": source})
            total = total + incoming[source].astype(jnp.float32)
        held[me_hot] = hidden_of(total, bits[me_hot], first_slot)
        for k, peer in enumerate(hot_peers):
            send(held.at[me_hot], held.at[me_hot], hg_send.at[s, index, k],
                 hg_recv.at[s, index, me_hot], {"hot": peer})

    for s in range(2):
        for k in range(chunks):
            finish(s, k, part_cold.at[s, k], got_cold.at[s, k], bits_cold.at[s],
                   hot_slots + k * (CHUNK // BLOCK), own_cold.at[s, k])
        finish(s, chunks, part_hot.at[s], got_hot.at[s], bits_hot.at[s], 0, own_hot.at[s])

    def gathered(s, index, held):
        for k in range(1, n_hot):
            source = lax.rem(me_hot + n_hot - k, n_hot)
            arrive(held.at[source], hg_send.at[s, index, k - 1], hg_recv.at[s, index, source],
                   {"hot": source})
        value = held[...].astype(jnp.float32)
        return value.reshape(value.shape[0] * value.shape[1], value.shape[2]).astype(jnp.bfloat16)

    def down(s):
        for k in range(chunks):
            full[s, :, hot_width + k * CHUNK:hot_width + (k + 1) * CHUNK] = dot(
                spread[s], gathered(s, k, own_cold.at[s, k])
            ).astype(jnp.bfloat16)
        full[s, :, :hot_width] = gathered(s, chunks, own_hot.at[s])
        if s == 0:
            for copy in loads[5 + 2 * chunks:]:
                copy.wait()
        for c in range(out_chunks):
            at = pl.ds(c * OUT_CHUNK, OUT_CHUNK)
            value = dot(full[s], w_down[:, c * OUT_CHUNK:(c + 1) * OUT_CHUNK])
            outs[s, :, :, :, at] = value.reshape(span, 2, rows, OUT_CHUNK)
            send(outs.at[s, :, 1 - my_side, :, at], pair_in.at[s, :, :, at],
                 pr_send.at[s, c], pr_recv.at[s, c], {"cold": other})

    def combine(s):
        for c in range(out_chunks):
            at = pl.ds(c * OUT_CHUNK, OUT_CHUNK)
            arrive(pair_in.at[s, :, :, at], pr_send.at[s, c], pr_recv.at[s, c], {"cold": other})
            value = outs[s, :, my_side, :, at] + pair_in[s, :, :, at]
            if s == 0:
                mine[:, :, at] = value
            ready[s, :, :, at] = value.astype(ready.dtype)
            for k, place in enumerate(places[s]):
                send(ready.at[s, place, :, at], final_in.at[my_pair, :, at],
                     fin_send.at[s, c, k], fin_recv.at[c, my_pair],
                     {"cold": (halves[s] * span + place) * 2 + my_side})

    for s in range(2):
        down(s)
        combine(s)
    for c in range(out_chunks):
        at = pl.ds(c * OUT_CHUNK, OUT_CHUNK)
        total = mine[my_place, :, at]
        for source in sources:
            arrive(final_in.at[source, :, at], fin_send.at[0, c, 0], fin_recv.at[c, source],
                   {"cold": source * 2 + my_side})
            total = total + final_in[source, :, at].astype(jnp.float32)
        out_ref[:, at] = total.astype(out_ref.dtype)
    for copy in sent:
        copy.wait_send()


def body(n_hot, n_cold, *args):
    (tokens, hot_gate, hot_up, hot_down, cold_gate, cold_up, cold_down,
     hot_ids, cold_ids, block_mask) = args
    rows, cols = tokens.shape
    total_rows = block_mask.shape[0]
    hot_width, cold_width = hot_gate.shape[1], cold_gate.shape[1]
    chunks = cold_width // CHUNK
    pairs = n_cold // 2
    span = pairs // 2
    stage_tokens, stage_picks = total_rows // 2, span * 2 * (rows // 2)
    slots_pad = -(-((hot_width + cold_width) // BLOCK) // 8) * 8
    hot_rows, cold_rows = stage_tokens // n_hot, stage_picks // n_hot
    out_chunks = cols // OUT_CHUNK
    bf16, f32, i32 = jnp.bfloat16, jnp.float32, jnp.int32
    vmem, dma = pltpu.VMEM, pltpu.SemaphoreType.DMA
    scratch = [
        vmem((total_rows, cols), bf16),
        vmem((cols, 2 * hot_width), bf16),
        vmem((chunks, cols, 2 * CHUNK), bf16),
        vmem((hot_width + cold_width, cols), bf16),
        pltpu.SMEM(hot_ids.shape, i32),
        pltpu.SMEM(cold_ids.shape, i32),
        vmem(block_mask.shape[::-1], i32),
        vmem((2, stage_picks, stage_tokens), bf16),
        vmem((2, stage_picks, cols), bf16),
        vmem((2, n_hot, hot_rows, slots_pad), f32),
        vmem((2, n_hot, cold_rows, slots_pad), f32),
        vmem((2, stage_tokens, stage_picks), bf16),
        vmem((2, n_hot, hot_rows, 2 * hot_width), f32),
        vmem((2, chunks, n_hot, cold_rows, 2 * CHUNK), f32),
        vmem((2, n_hot, hot_rows, 2 * hot_width), SUM_TYPE),
        vmem((2, chunks, n_hot, cold_rows, 2 * CHUNK), SUM_TYPE),
        vmem((2, n_hot, hot_rows, 2 * hot_width), SUM_TYPE),
        vmem((2, chunks, n_hot, cold_rows, 2 * CHUNK), SUM_TYPE),
        vmem((2, n_hot, hot_rows, hot_width), bf16),
        vmem((2, chunks, n_hot, cold_rows, CHUNK), bf16),
        vmem((2, stage_tokens, hot_width + cold_width), bf16),
        vmem((2, span, 2, rows, cols), f32),
        vmem((2, span, rows, cols), f32),
        vmem((span, rows, cols), f32),
        vmem((2, span, rows, cols), OUT_TYPE),
        vmem((pairs, rows, cols), OUT_TYPE),
        dma((7 + 2 * chunks,)),
        dma,
        dma((pairs,)),
        dma((pairs,)),
        dma((pairs,)),
        dma((pairs,)),
        dma((2, chunks + 1, n_hot)),
        dma((2, chunks + 1, n_hot)),
        dma((2, chunks + 1, n_hot)),
        dma((2, chunks + 1, n_hot)),
        dma((2, out_chunks)),
        dma((2, out_chunks)),
        dma((2, out_chunks, span)),
        dma((out_chunks, pairs)),
    ]
    return pl.pallas_call(
        functools.partial(kernel, n_hot, n_cold),
        out_shape=jax.ShapeDtypeStruct((rows, cols), bf16),
        in_specs=[pl.BlockSpec(memory_space=pl.ANY)] * 10,
        out_specs=pl.BlockSpec(memory_space=pltpu.VMEM),
        scratch_shapes=scratch,
        compiler_params=pltpu.CompilerParams(
            collective_id=0, has_side_effects=True, vmem_limit_bytes=60 * 1024 * 1024
        ),
        name="decode_step",
    )(*args[:-1], block_mask.T)


def solution(mesh):
    return jax.shard_map(
        functools.partial(body, mesh.shape["hot"], mesh.shape["cold"]),
        mesh=mesh,
        in_specs=(
            P("cold", "hot"),
            P("hot", "cold"),
            P("hot", "cold"),
            P("cold", "hot"),
            P("hot", "cold"),
            P("hot", "cold"),
            P("cold", "hot"),
            P(),
            P(),
            P(),
        ),
        out_specs=P("cold", "hot"),
        check_vma=False,
    )
```

```python
import functools

import jax
import jax.numpy as jnp
from jax import lax
from jax.experimental import pallas as pl
from jax.experimental.pallas import tpu as pltpu
from jax.sharding import PartitionSpec as P

BLOCK = 128
CHUNK = 256
OUT_CHUNK = 1024
MESH = pl.DeviceIdType.MESH
NT = (((1,), (1,)), ((), ()))
SUM_TYPE = jnp.bfloat16
OUT_TYPE = jnp.bfloat16


def dot(a, b):
    return jnp.dot(a, b, preferred_element_type=jnp.float32)


def dot_nt(a, b):
    return lax.dot_general(a, b, NT, preferred_element_type=jnp.float32)


def zero_one(condition):
    return jnp.where(condition, 1.0, 0.0).astype(jnp.bfloat16)


def hidden_of(sums, bits, first_slot):
    width = sums.shape[1] // 2
    gate, up = sums[:, :width], sums[:, width:]
    value = gate / (1.0 + jnp.exp(-gate)) * up
    pieces = [
        value[:, j * BLOCK:(j + 1) * BLOCK] * bits[:, first_slot + j:first_slot + j + 1]
        for j in range(width // BLOCK)
    ]
    return jnp.concatenate(pieces, axis=1).astype(jnp.bfloat16)


def kernel(
    n_hot, n_cold,
    tok_in, hg_in, hu_in, hd_in, cg_in, cu_in, cd_in, hid_in, cid_in, mask_in,
    out_ref,
    tok_all, w_hot, w_cold, w_down, hot_ids, cold_ids, mask,
    picked, bits_hot, bits_cold, spread,
    part_hot, part_cold, send_hot, send_cold, got_hot, got_cold,
    own_hot, own_cold, full, outs, pair_in, mine, ready, final_in,
    load_sem, tok_sem, tok_send, tok_recv, fwd_send, fwd_recv,
    rs_send, rs_recv, hg_send, hg_recv, pr_send, pr_recv, fin_send, fin_recv,
):
    me_hot, me_cold = lax.axis_index("hot"), lax.axis_index("cold")
    pairs = n_cold // 2
    my_pair, my_side = me_cold // 2, me_cold % 2
    other = my_pair * 2 + (1 - my_side)
    rows = tok_in.shape[0]
    tokens = tok_all.shape[0]
    hot_width = hg_in.shape[1]
    hot_slots = hot_width // BLOCK
    cold_width = cg_in.shape[1]
    cold_slots = cold_width // BLOCK
    chunks = cold_width // CHUNK
    slot_count = rows // 2
    picks = n_cold * slot_count
    hot_rows, cold_rows = tokens // n_hot, picks // n_hot
    cols = tok_in.shape[1]
    out_chunks = cols // OUT_CHUNK

    own_slot = tok_all.at[pl.ds(pl.multiple_of(me_cold * rows, rows), rows)]
    tok_load = pltpu.make_async_copy(tok_in, own_slot, tok_sem)
    tok_load.start()
    loads = []

    def load(src, dst):
        copy = pltpu.make_async_copy(src, dst, load_sem.at[len(loads)])
        copy.start()
        loads.append(copy)

    load(hid_in, hot_ids)
    load(cid_in, cold_ids)
    load(mask_in, mask)
    barrier = pltpu.get_barrier_semaphore()
    way = 2 * (me_hot // (n_hot // 2)) - 1
    hot_peers = [lax.rem(me_hot + way * k + n_hot, n_hot) for k in range(1, n_hot)]
    span = pairs // 2
    my_half, my_place = my_pair // span, my_pair % span
    far, near = (1 - my_half) * span, my_half * span
    pair_peers = [far + lax.rem(my_place + k, span) for k in range(1, span)]
    pair_peers += [near + lax.rem(my_place + k, span) for k in range(1, span)] + [far + my_place]
    sources = [far + my_place]
    sources += [far + lax.rem(my_place + span - k, span) for k in range(1, span)]
    sources += [near + lax.rem(my_place + span - k, span) for k in range(1, span)]
    for peer in hot_peers:
        pl.semaphore_signal(barrier, inc=1, device_id={"hot": peer}, device_id_type=MESH)
    for peer in pair_peers:
        pl.semaphore_signal(
            barrier, inc=1, device_id={"cold": peer * 2 + my_side}, device_id_type=MESH
        )
    pl.semaphore_signal(barrier, inc=1, device_id={"cold": other}, device_id_type=MESH)
    for copy in loads[:3]:
        copy.wait()
    slots_pad = bits_hot.shape[1]
    blocks = mask.shape[0]
    slot_at = lax.broadcasted_iota(jnp.int32, (slots_pad, blocks), 0)
    id_at = jnp.full((slots_pad, blocks), -1, jnp.int32)
    for j in range(hot_slots):
        id_at = jnp.where(slot_at == j, hot_ids[me_cold * hot_slots + j], id_at)
    for j in range(cold_slots):
        id_at = jnp.where(slot_at == hot_slots + j, cold_ids[me_cold * cold_slots + j], id_at)
    chosen = zero_one(lax.broadcasted_iota(jnp.int32, (slots_pad, blocks), 1) == id_at)
    mask_value = mask[...].astype(jnp.float32).astype(jnp.bfloat16)
    bits_t = dot(chosen, mask_value)
    slot_row = lax.broadcasted_iota(jnp.int32, (slots_pad, tokens), 0)
    is_cold = (slot_row >= hot_slots) & (slot_row < hot_slots + cold_slots)
    hit = jnp.max(jnp.where(is_cold, bits_t, 0.0), axis=0, keepdims=True)

    def group_of(shape, dim):
        at = lax.broadcasted_iota(jnp.int32, shape, dim)
        total = jnp.zeros(shape, jnp.int32)
        for g in range(1, n_cold):
            total = total + jnp.where(at >= g * rows, 1, 0)
        return total

    group_row, group_col = group_of((1, tokens), 1), group_of((tokens, 1), 0)
    before = lax.broadcasted_iota(jnp.int32, (tokens, tokens), 0) < lax.broadcasted_iota(
        jnp.int32, (tokens, tokens), 1
    )
    before = zero_one(before & (group_row == group_col))
    rank = dot(jnp.broadcast_to(hit, (8, tokens)).astype(jnp.bfloat16), before)[0:1]
    target = jnp.where(hit > 0.5, group_row * slot_count + rank.astype(jnp.int32), -1)
    pick = zero_one(lax.broadcasted_iota(jnp.int32, (picks, tokens), 0) == target)
    eye = zero_one(
        lax.broadcasted_iota(jnp.int32, (tokens, tokens), 0)
        == lax.broadcasted_iota(jnp.int32, (tokens, tokens), 1)
    )
    spread[...] = dot_nt(eye, pick).astype(jnp.bfloat16)
    bits_cold[...] = dot_nt(pick, bits_t.astype(jnp.bfloat16))
    bits_hot[...] = dot_nt(eye, bits_t.astype(jnp.bfloat16))

    pl.semaphore_wait(barrier, n_hot - 1 + pairs - 1 + 1)

    sent = []

    def send(src, dst, s_sem, r_sem, device):
        copy = pltpu.make_async_remote_copy(
            src_ref=src, dst_ref=dst, send_sem=s_sem, recv_sem=r_sem,
            device_id=device, device_id_type=MESH,
        )
        copy.start()
        sent.append(copy)

    def arrive(dst, s_sem, r_sem, device):
        pltpu.make_async_remote_copy(
            src_ref=dst, dst_ref=dst, send_sem=s_sem, recv_sem=r_sem,
            device_id=device, device_id_type=MESH,
        ).wait_recv()

    tok_load.wait()
    for k, peer in enumerate(pair_peers):
        send(own_slot, own_slot, tok_send.at[k], tok_recv.at[my_pair],
             {"cold": peer * 2 + my_side})
    send(own_slot, own_slot, fwd_send.at[0], fwd_recv.at[my_pair], {"cold": other})

    load(hg_in, w_hot.at[:, pl.ds(0, hot_width)])
    load(hu_in, w_hot.at[:, pl.ds(hot_width, hot_width)])
    for k in range(chunks):
        load(cg_in.at[:, pl.ds(k * CHUNK, CHUNK)], w_cold.at[k, :, pl.ds(0, CHUNK)])
        load(cu_in.at[:, pl.ds(k * CHUNK, CHUNK)], w_cold.at[k, :, pl.ds(CHUNK, CHUNK)])
    load(hd_in, w_down.at[pl.ds(0, hot_width)])
    load(cd_in, w_down.at[pl.ds(hot_width, cold_width)])

    def slot_of(device):
        return tok_all.at[pl.ds(pl.multiple_of(device * rows, rows), rows)]

    for k, source in enumerate(sources, 1):
        slot = slot_of(source * 2 + my_side)
        arrive(slot, tok_send.at[k - 1], tok_recv.at[source], {"cold": source * 2 + my_side})
        send(slot, slot, fwd_send.at[k], fwd_recv.at[source], {"cold": other})
    for k, source in enumerate([my_pair] + sources):
        arrive(slot_of(source * 2 + (1 - my_side)), fwd_send.at[k], fwd_recv.at[source],
               {"cold": other})

    def part(index, value, kept, outgoing, incoming, count):
        kept[...] = value
        if outgoing is not kept:
            outgoing[...] = value.astype(outgoing.dtype)
        for k, peer in enumerate(hot_peers):
            send(
                outgoing.at[pl.ds(pl.multiple_of(peer * count, count), count)],
                incoming.at[me_hot],
                rs_send.at[index, k], rs_recv.at[index, me_hot], {"hot": peer},
            )

    loads[3].wait()
    loads[4].wait()
    picked[...] = dot(pick, tok_all[...]).astype(jnp.bfloat16)
    for k in range(chunks):
        loads[5 + 2 * k].wait()
        loads[6 + 2 * k].wait()
        part(k, dot(picked[...], w_cold[k]), part_cold.at[k], send_cold.at[k],
             got_cold.at[k], cold_rows)
    part(chunks, dot(tok_all[...], w_hot[...]), part_hot, send_hot, got_hot, hot_rows)

    def finish(index, kept, incoming, count, bits, first_slot, held):
        own = pl.ds(pl.multiple_of(me_hot * count, count), count)
        total = kept[own]
        for k in range(1, n_hot):
            source = lax.rem(me_hot + n_hot - k, n_hot)
            arrive(incoming.at[source], rs_send.at[index, k - 1], rs_recv.at[index, source],
                   {"hot": source})
            total = total + incoming[source].astype(jnp.float32)
        held[own] = hidden_of(total, bits[own], first_slot)
        for k, peer in enumerate(hot_peers):
            send(held.at[own], held.at[own], hg_send.at[index, k], hg_recv.at[index, me_hot],
                 {"hot": peer})

    for k in range(chunks):
        finish(k, part_cold.at[k], got_cold.at[k], cold_rows, bits_cold,
               hot_slots + k * (CHUNK // BLOCK), own_cold.at[k])
    finish(chunks, part_hot, got_hot, hot_rows, bits_hot, 0, own_hot)

    def gathered(index, count, held):
        for k in range(1, n_hot):
            source = lax.rem(me_hot + n_hot - k, n_hot)
            arrive(held.at[pl.ds(pl.multiple_of(source * count, count), count)],
                   hg_send.at[index, k - 1], hg_recv.at[index, source], {"hot": source})

    for k in range(chunks):
        gathered(k, cold_rows, own_cold.at[k])
        full[:, hot_width + k * CHUNK:hot_width + (k + 1) * CHUNK] = dot(
            spread[...], own_cold[k]
        ).astype(jnp.bfloat16)
    gathered(chunks, hot_rows, own_hot)
    full[:, :hot_width] = own_hot[...]

    for copy in loads[5 + 2 * chunks:]:
        copy.wait()
    for c in range(out_chunks):
        at = pl.ds(c * OUT_CHUNK, OUT_CHUNK)
        value = dot(full[...], w_down[:, c * OUT_CHUNK:(c + 1) * OUT_CHUNK])
        outs[:, :, :, at] = value.reshape(pairs, 2, rows, OUT_CHUNK)
        send(outs.at[:, 1 - my_side, :, at], pair_in.at[:, :, at],
             pr_send.at[c], pr_recv.at[c], {"cold": other})
    for c in range(out_chunks):
        at = pl.ds(c * OUT_CHUNK, OUT_CHUNK)
        arrive(pair_in.at[:, :, at], pr_send.at[c], pr_recv.at[c], {"cold": other})
        value = outs[:, my_side, :, at] + pair_in[:, :, at]
        mine[:, :, at] = value
        ready[:, :, at] = value.astype(ready.dtype)
        for k, peer in enumerate(pair_peers):
            send(ready.at[peer, :, at], final_in.at[my_pair, :, at],
                 fin_send.at[c, k], fin_recv.at[c, my_pair], {"cold": peer * 2 + my_side})
    for c in range(out_chunks):
        at = pl.ds(c * OUT_CHUNK, OUT_CHUNK)
        total = mine[my_pair, :, at]
        for k, source in enumerate(sources, 1):
            arrive(final_in.at[source, :, at], fin_send.at[c, k - 1], fin_recv.at[c, source],
                   {"cold": source * 2 + my_side})
            total = total + final_in[source, :, at].astype(jnp.float32)
        out_ref[:, at] = total.astype(out_ref.dtype)
    for copy in sent:
        copy.wait_send()


def body(n_hot, n_cold, *args):
    (tokens, hot_gate, hot_up, hot_down, cold_gate, cold_up, cold_down,
     hot_ids, cold_ids, block_mask) = args
    rows, cols = tokens.shape
    total_rows = block_mask.shape[0]
    hot_width, cold_width = hot_gate.shape[1], cold_gate.shape[1]
    chunks = cold_width // CHUNK
    picks = n_cold * (rows // 2)
    pairs = n_cold // 2
    slots_pad = -(-((hot_width + cold_width) // BLOCK) // 8) * 8
    hot_rows, cold_rows = total_rows // n_hot, picks // n_hot
    out_chunks = cols // OUT_CHUNK
    bf16, f32, i32 = jnp.bfloat16, jnp.float32, jnp.int32
    vmem, dma = pltpu.VMEM, pltpu.SemaphoreType.DMA
    scratch = [
        vmem((total_rows, cols), bf16),
        vmem((cols, 2 * hot_width), bf16),
        vmem((chunks, cols, 2 * CHUNK), bf16),
        vmem((hot_width + cold_width, cols), bf16),
        pltpu.SMEM(hot_ids.shape, i32),
        pltpu.SMEM(cold_ids.shape, i32),
        vmem(block_mask.shape[::-1], i32),
        vmem((picks, cols), bf16),
        vmem((total_rows, slots_pad), f32),
        vmem((picks, slots_pad), f32),
        vmem((total_rows, picks), bf16),
        vmem((total_rows, 2 * hot_width), f32),
        vmem((chunks, picks, 2 * CHUNK), f32),
        vmem((total_rows, 2 * hot_width), SUM_TYPE),
        vmem((chunks, picks, 2 * CHUNK), SUM_TYPE),
        vmem((n_hot, hot_rows, 2 * hot_width), SUM_TYPE),
        vmem((chunks, n_hot, cold_rows, 2 * CHUNK), SUM_TYPE),
        vmem((total_rows, hot_width), bf16),
        vmem((chunks, picks, CHUNK), bf16),
        vmem((total_rows, hot_width + cold_width), bf16),
        vmem((pairs, 2, rows, cols), f32),
        vmem((pairs, rows, cols), f32),
        vmem((pairs, rows, cols), f32),
        vmem((pairs, rows, cols), OUT_TYPE),
        vmem((pairs, rows, cols), OUT_TYPE),
        dma((7 + 2 * chunks,)),
        dma,
        dma((pairs,)),
        dma((pairs,)),
        dma((pairs,)),
        dma((pairs,)),
        dma((chunks + 1, n_hot)),
        dma((chunks + 1, n_hot)),
        dma((chunks + 1, n_hot)),
        dma((chunks + 1, n_hot)),
        dma((out_chunks,)),
        dma((out_chunks,)),
        dma((out_chunks, pairs)),
        dma((out_chunks, pairs)),
    ]
    return pl.pallas_call(
        functools.partial(kernel, n_hot, n_cold),
        out_shape=jax.ShapeDtypeStruct((rows, cols), bf16),
        in_specs=[pl.BlockSpec(memory_space=pl.ANY)] * 10,
        out_specs=pl.BlockSpec(memory_space=pltpu.VMEM),
        scratch_shapes=scratch,
        compiler_params=pltpu.CompilerParams(
            collective_id=0, has_side_effects=True, vmem_limit_bytes=60 * 1024 * 1024
        ),
        name="decode_step",
    )(*args[:-1], block_mask.T)


def solution(mesh):
    return jax.shard_map(
        functools.partial(body, mesh.shape["hot"], mesh.shape["cold"]),
        mesh=mesh,
        in_specs=(
            P("cold", "hot"),
            P("hot", "cold"),
            P("hot", "cold"),
            P("cold", "hot"),
            P("hot", "cold"),
            P("hot", "cold"),
            P("cold", "hot"),
            P(),
            P(),
            P(),
        ),
        out_specs=P("cold", "hot"),
        check_vma=False,
    )
```

```python
import functools

import jax
import jax.numpy as jnp
from jax import lax
from jax.experimental import pallas as pl
from jax.experimental.pallas import tpu as pltpu
from jax.sharding import PartitionSpec as P

BLOCK = 128
CHUNK = 256
OUT_CHUNK = 1024
MESH = pl.DeviceIdType.MESH
NT = (((1,), (1,)), ((), ()))
SUM_TYPE = jnp.bfloat16
OUT_TYPE = jnp.bfloat16


def dot(a, b):
    return jnp.dot(a, b, preferred_element_type=jnp.float32)


def dot_nt(a, b):
    return lax.dot_general(a, b, NT, preferred_element_type=jnp.float32)


def zero_one(condition):
    return jnp.where(condition, 1.0, 0.0).astype(jnp.bfloat16)


def hidden_of(sums, bits, first_slot):
    width = sums.shape[1] // 2
    gate, up = sums[:, :width], sums[:, width:]
    value = gate / (1.0 + jnp.exp(-gate)) * up
    pieces = [
        value[:, j * BLOCK:(j + 1) * BLOCK] * bits[:, first_slot + j:first_slot + j + 1]
        for j in range(width // BLOCK)
    ]
    return jnp.concatenate(pieces, axis=1).astype(jnp.bfloat16)


def kernel(
    n_hot, n_cold,
    tok_in, hg_in, hu_in, hd_in, cg_in, cu_in, cd_in, hid_in, cid_in, mask_in,
    out_ref,
    tok_all, w_hot, w_cold, w_down, hot_ids, cold_ids, mask,
    picked, bits_hot, bits_cold, spread,
    part_hot, part_cold, send_hot, send_cold, got_hot, got_cold,
    own_hot, own_cold, full, outs, pair_in, mine, ready, final_in,
    load_sem, tok_sem, tok_send, tok_recv, fwd_send, fwd_recv,
    rs_send, rs_recv, hg_send, hg_recv, pr_send, pr_recv, fin_send, fin_recv,
):
    me_hot, me_cold = lax.axis_index("hot"), lax.axis_index("cold")
    pairs = n_cold // 2
    my_pair, my_side = me_cold // 2, me_cold % 2
    other = my_pair * 2 + (1 - my_side)
    rows = tok_in.shape[0]
    tokens = tok_all.shape[0]
    hot_width = hg_in.shape[1]
    hot_slots = hot_width // BLOCK
    cold_width = cg_in.shape[1]
    cold_slots = cold_width // BLOCK
    chunks = cold_width // CHUNK
    slot_count = rows // 2
    picks = n_cold * slot_count
    hot_rows, cold_rows = tokens // n_hot, picks // n_hot
    cols = tok_in.shape[1]
    out_chunks = cols // OUT_CHUNK

    own_slot = tok_all.at[pl.ds(pl.multiple_of(me_cold * rows, rows), rows)]
    tok_load = pltpu.make_async_copy(tok_in, own_slot, tok_sem)
    tok_load.start()
    loads = []

    def load(src, dst):
        copy = pltpu.make_async_copy(src, dst, load_sem.at[len(loads)])
        copy.start()
        loads.append(copy)

    load(hid_in, hot_ids)
    load(cid_in, cold_ids)
    load(mask_in, mask)
    barrier = pltpu.get_barrier_semaphore()
    hot_peers = [lax.rem(me_hot + k, n_hot) for k in range(1, n_hot)]
    pair_peers = [lax.rem(my_pair + k, pairs) for k in range(1, pairs)]
    for peer in hot_peers:
        pl.semaphore_signal(barrier, inc=1, device_id={"hot": peer}, device_id_type=MESH)
    for peer in pair_peers:
        pl.semaphore_signal(
            barrier, inc=1, device_id={"cold": peer * 2 + my_side}, device_id_type=MESH
        )
    pl.semaphore_signal(barrier, inc=1, device_id={"cold": other}, device_id_type=MESH)
    for copy in loads[:3]:
        copy.wait()
    slots_pad = bits_hot.shape[1]
    blocks = mask.shape[0]
    slot_at = lax.broadcasted_iota(jnp.int32, (slots_pad, blocks), 0)
    id_at = jnp.full((slots_pad, blocks), -1, jnp.int32)
    for j in range(hot_slots):
        id_at = jnp.where(slot_at == j, hot_ids[me_cold * hot_slots + j], id_at)
    for j in range(cold_slots):
        id_at = jnp.where(slot_at == hot_slots + j, cold_ids[me_cold * cold_slots + j], id_at)
    chosen = zero_one(lax.broadcasted_iota(jnp.int32, (slots_pad, blocks), 1) == id_at)
    mask_value = mask[...].astype(jnp.float32).astype(jnp.bfloat16)
    bits_t = dot(chosen, mask_value)
    slot_row = lax.broadcasted_iota(jnp.int32, (slots_pad, tokens), 0)
    is_cold = (slot_row >= hot_slots) & (slot_row < hot_slots + cold_slots)
    hit = jnp.max(jnp.where(is_cold, bits_t, 0.0), axis=0, keepdims=True)

    def group_of(shape, dim):
        at = lax.broadcasted_iota(jnp.int32, shape, dim)
        total = jnp.zeros(shape, jnp.int32)
        for g in range(1, n_cold):
            total = total + jnp.where(at >= g * rows, 1, 0)
        return total

    group_row, group_col = group_of((1, tokens), 1), group_of((tokens, 1), 0)
    before = lax.broadcasted_iota(jnp.int32, (tokens, tokens), 0) < lax.broadcasted_iota(
        jnp.int32, (tokens, tokens), 1
    )
    before = zero_one(before & (group_row == group_col))
    rank = dot(jnp.broadcast_to(hit, (8, tokens)).astype(jnp.bfloat16), before)[0:1]
    target = jnp.where(hit > 0.5, group_row * slot_count + rank.astype(jnp.int32), -1)
    pick = zero_one(lax.broadcasted_iota(jnp.int32, (picks, tokens), 0) == target)
    eye = zero_one(
        lax.broadcasted_iota(jnp.int32, (tokens, tokens), 0)
        == lax.broadcasted_iota(jnp.int32, (tokens, tokens), 1)
    )
    spread[...] = dot_nt(eye, pick).astype(jnp.bfloat16)
    bits_cold[...] = dot_nt(pick, bits_t.astype(jnp.bfloat16))
    bits_hot[...] = dot_nt(eye, bits_t.astype(jnp.bfloat16))

    pl.semaphore_wait(barrier, n_hot - 1 + pairs - 1 + 1)

    sent = []

    def send(src, dst, s_sem, r_sem, device):
        copy = pltpu.make_async_remote_copy(
            src_ref=src, dst_ref=dst, send_sem=s_sem, recv_sem=r_sem,
            device_id=device, device_id_type=MESH,
        )
        copy.start()
        sent.append(copy)

    def arrive(dst, s_sem, r_sem, device):
        pltpu.make_async_remote_copy(
            src_ref=dst, dst_ref=dst, send_sem=s_sem, recv_sem=r_sem,
            device_id=device, device_id_type=MESH,
        ).wait_recv()

    tok_load.wait()
    for k, peer in enumerate(pair_peers):
        send(own_slot, own_slot, tok_send.at[k], tok_recv.at[my_pair],
             {"cold": peer * 2 + my_side})
    send(own_slot, own_slot, fwd_send.at[0], fwd_recv.at[my_pair], {"cold": other})

    load(hg_in, w_hot.at[:, pl.ds(0, hot_width)])
    load(hu_in, w_hot.at[:, pl.ds(hot_width, hot_width)])
    for k in range(chunks):
        load(cg_in.at[:, pl.ds(k * CHUNK, CHUNK)], w_cold.at[k, :, pl.ds(0, CHUNK)])
        load(cu_in.at[:, pl.ds(k * CHUNK, CHUNK)], w_cold.at[k, :, pl.ds(CHUNK, CHUNK)])
    load(hd_in, w_down.at[pl.ds(0, hot_width)])
    load(cd_in, w_down.at[pl.ds(hot_width, cold_width)])

    def slot_of(device):
        return tok_all.at[pl.ds(pl.multiple_of(device * rows, rows), rows)]

    for k in range(1, pairs):
        source = lax.rem(my_pair + pairs - k, pairs)
        slot = slot_of(source * 2 + my_side)
        arrive(slot, tok_send.at[k - 1], tok_recv.at[source], {"cold": source * 2 + my_side})
        send(slot, slot, fwd_send.at[k], fwd_recv.at[source], {"cold": other})
    for k in range(pairs):
        source = lax.rem(my_pair + pairs - k, pairs)
        arrive(slot_of(source * 2 + (1 - my_side)), fwd_send.at[k], fwd_recv.at[source],
               {"cold": other})

    def part(index, value, kept, outgoing, incoming, count):
        kept[...] = value
        if outgoing is not kept:
            outgoing[...] = value.astype(outgoing.dtype)
        for k, peer in enumerate(hot_peers):
            send(
                outgoing.at[pl.ds(pl.multiple_of(peer * count, count), count)],
                incoming.at[me_hot],
                rs_send.at[index, k], rs_recv.at[index, me_hot], {"hot": peer},
            )

    loads[3].wait()
    loads[4].wait()
    picked[...] = dot(pick, tok_all[...]).astype(jnp.bfloat16)
    for k in range(chunks):
        loads[5 + 2 * k].wait()
        loads[6 + 2 * k].wait()
        part(k, dot(picked[...], w_cold[k]), part_cold.at[k], send_cold.at[k],
             got_cold.at[k], cold_rows)
    part(chunks, dot(tok_all[...], w_hot[...]), part_hot, send_hot, got_hot, hot_rows)

    def finish(index, kept, incoming, count, bits, first_slot, held):
        own = pl.ds(pl.multiple_of(me_hot * count, count), count)
        total = kept[own]
        for k in range(1, n_hot):
            source = lax.rem(me_hot + n_hot - k, n_hot)
            arrive(incoming.at[source], rs_send.at[index, k - 1], rs_recv.at[index, source],
                   {"hot": source})
            total = total + incoming[source].astype(jnp.float32)
        held[own] = hidden_of(total, bits[own], first_slot)
        for k, peer in enumerate(hot_peers):
            send(held.at[own], held.at[own], hg_send.at[index, k], hg_recv.at[index, me_hot],
                 {"hot": peer})

    for k in range(chunks):
        finish(k, part_cold.at[k], got_cold.at[k], cold_rows, bits_cold,
               hot_slots + k * (CHUNK // BLOCK), own_cold.at[k])
    finish(chunks, part_hot, got_hot, hot_rows, bits_hot, 0, own_hot)

    def gathered(index, count, held):
        for k in range(1, n_hot):
            source = lax.rem(me_hot + n_hot - k, n_hot)
            arrive(held.at[pl.ds(pl.multiple_of(source * count, count), count)],
                   hg_send.at[index, k - 1], hg_recv.at[index, source], {"hot": source})

    for k in range(chunks):
        gathered(k, cold_rows, own_cold.at[k])
        full[:, hot_width + k * CHUNK:hot_width + (k + 1) * CHUNK] = dot(
            spread[...], own_cold[k]
        ).astype(jnp.bfloat16)
    gathered(chunks, hot_rows, own_hot)
    full[:, :hot_width] = own_hot[...]

    for copy in loads[5 + 2 * chunks:]:
        copy.wait()
    for c in range(out_chunks):
        at = pl.ds(c * OUT_CHUNK, OUT_CHUNK)
        value = dot(full[...], w_down[:, c * OUT_CHUNK:(c + 1) * OUT_CHUNK])
        outs[:, :, :, at] = value.reshape(pairs, 2, rows, OUT_CHUNK)
        send(outs.at[:, 1 - my_side, :, at], pair_in.at[:, :, at],
             pr_send.at[c], pr_recv.at[c], {"cold": other})
    for c in range(out_chunks):
        at = pl.ds(c * OUT_CHUNK, OUT_CHUNK)
        arrive(pair_in.at[:, :, at], pr_send.at[c], pr_recv.at[c], {"cold": other})
        value = outs[:, my_side, :, at] + pair_in[:, :, at]
        mine[:, :, at] = value
        ready[:, :, at] = value.astype(ready.dtype)
        for k, peer in enumerate(pair_peers):
            send(ready.at[peer, :, at], final_in.at[my_pair, :, at],
                 fin_send.at[c, k], fin_recv.at[c, my_pair], {"cold": peer * 2 + my_side})
    for c in range(out_chunks):
        at = pl.ds(c * OUT_CHUNK, OUT_CHUNK)
        total = mine[my_pair, :, at]
        for k in range(1, pairs):
            source = lax.rem(my_pair + pairs - k, pairs)
            arrive(final_in.at[source, :, at], fin_send.at[c, k - 1], fin_recv.at[c, source],
                   {"cold": source * 2 + my_side})
            total = total + final_in[source, :, at].astype(jnp.float32)
        out_ref[:, at] = total.astype(out_ref.dtype)
    for copy in sent:
        copy.wait_send()


def body(n_hot, n_cold, *args):
    (tokens, hot_gate, hot_up, hot_down, cold_gate, cold_up, cold_down,
     hot_ids, cold_ids, block_mask) = args
    rows, cols = tokens.shape
    total_rows = block_mask.shape[0]
    hot_width, cold_width = hot_gate.shape[1], cold_gate.shape[1]
    chunks = cold_width // CHUNK
    picks = n_cold * (rows // 2)
    pairs = n_cold // 2
    slots_pad = -(-((hot_width + cold_width) // BLOCK) // 8) * 8
    hot_rows, cold_rows = total_rows // n_hot, picks // n_hot
    out_chunks = cols // OUT_CHUNK
    bf16, f32, i32 = jnp.bfloat16, jnp.float32, jnp.int32
    vmem, dma = pltpu.VMEM, pltpu.SemaphoreType.DMA
    scratch = [
        vmem((total_rows, cols), bf16),
        vmem((cols, 2 * hot_width), bf16),
        vmem((chunks, cols, 2 * CHUNK), bf16),
        vmem((hot_width + cold_width, cols), bf16),
        pltpu.SMEM(hot_ids.shape, i32),
        pltpu.SMEM(cold_ids.shape, i32),
        vmem(block_mask.shape[::-1], i32),
        vmem((picks, cols), bf16),
        vmem((total_rows, slots_pad), f32),
        vmem((picks, slots_pad), f32),
        vmem((total_rows, picks), bf16),
        vmem((total_rows, 2 * hot_width), f32),
        vmem((chunks, picks, 2 * CHUNK), f32),
        vmem((total_rows, 2 * hot_width), SUM_TYPE),
        vmem((chunks, picks, 2 * CHUNK), SUM_TYPE),
        vmem((n_hot, hot_rows, 2 * hot_width), SUM_TYPE),
        vmem((chunks, n_hot, cold_rows, 2 * CHUNK), SUM_TYPE),
        vmem((total_rows, hot_width), bf16),
        vmem((chunks, picks, CHUNK), bf16),
        vmem((total_rows, hot_width + cold_width), bf16),
        vmem((pairs, 2, rows, cols), f32),
        vmem((pairs, rows, cols), f32),
        vmem((pairs, rows, cols), f32),
        vmem((pairs, rows, cols), OUT_TYPE),
        vmem((pairs, rows, cols), OUT_TYPE),
        dma((7 + 2 * chunks,)),
        dma,
        dma((pairs,)),
        dma((pairs,)),
        dma((pairs,)),
        dma((pairs,)),
        dma((chunks + 1, n_hot)),
        dma((chunks + 1, n_hot)),
        dma((chunks + 1, n_hot)),
        dma((chunks + 1, n_hot)),
        dma((out_chunks,)),
        dma((out_chunks,)),
        dma((out_chunks, pairs)),
        dma((out_chunks, pairs)),
    ]
    return pl.pallas_call(
        functools.partial(kernel, n_hot, n_cold),
        out_shape=jax.ShapeDtypeStruct((rows, cols), bf16),
        in_specs=[pl.BlockSpec(memory_space=pl.ANY)] * 10,
        out_specs=pl.BlockSpec(memory_space=pltpu.VMEM),
        scratch_shapes=scratch,
        compiler_params=pltpu.CompilerParams(
            collective_id=0, has_side_effects=True, vmem_limit_bytes=60 * 1024 * 1024
        ),
        name="decode_step",
    )(*args[:-1], block_mask.T)


def solution(mesh):
    return jax.shard_map(
        functools.partial(body, mesh.shape["hot"], mesh.shape["cold"]),
        mesh=mesh,
        in_specs=(
            P("cold", "hot"),
            P("hot", "cold"),
            P("hot", "cold"),
            P("cold", "hot"),
            P("hot", "cold"),
            P("hot", "cold"),
            P("cold", "hot"),
            P(),
            P(),
            P(),
        ),
        out_specs=P("cold", "hot"),
        check_vma=False,
    )
```
